32 devices in a mesh: groups: 2 (over y), tmpl: 8 (over z, x), det: 2 (over core).
Axes of the slice: x: 2, y: 2, z: 4, core: 2. Of those that a mesh axis runs over, the one named last changes fastest.
Arguments:
- basis_series: bfloat16 [3, 128, 32768], P(None, None, ('groups', 'tmpl', 'det')), parts along dimension 2, may hold values from -6 to 6
- reconstruction: bfloat16 [3, 256, 2, 128], P(None, ('groups', 'tmpl')), parts along dimension 1, may hold values from -0.5 to 0.5
- offsets: int32 [6], P('groups'), parts along dimension 0, may hold values from 1024 to 16383
Outputs:
- window_peaks: float32 [128, 256], P(None, ('groups', 'tmpl', 'det')), parts along dimension 1
The draws below stay inside these ranges and needn't reach their ends.
There are 2 independent parts, one for each index of `groups`. The reference program is written for one: setup_inputs(seed, part) draws one part's arguments, and reference() takes and returns one part's arrays. A program takes and returns all parts, laid end to end along the dimension named above; each array names one. Nothing has to cross between parts.
Inputs may be any that keep to these rules, and one draw needn't show every extreme that they name: `offsets`: slides are applied circularly over the segment's 16384 samples.
All inputs are finite; a program needn't handle non-finite values.
Results may differ from the reference program's by a relative error of at most 0.0003.
Values may be sent and summed in bfloat16 or wider, within the bound.
A program may use at most 64 MiB of HBM per device.

```python
import jax
import jax.numpy as jnp
from jax import lax

DETS = 3
BASIS = 128
WIN = 128
T_DEV = 1024
MAXQ = 16
TEMPL = 128
NT = 16384
NWIN = 128


def level_of(key, dims, pieces, low, top_value):
    factor_of = 1.0
    for axis_at, shards_of in pieces:
        steps = jax.random.uniform(jax.random.fold_in(jax.random.fold_in(key, 6), axis_at), (shards_of,), jnp.float32, low / len(pieces), top_value / len(pieces))
        factor_of = factor_of * jnp.repeat(jnp.exp(steps), dims[axis_at] // shards_of).reshape((-1,) + (1,) * (len(dims) - 1 - axis_at))
    return factor_of


def bell_draw(key, shape, spread, limit, pieces=(), dtype=jnp.bfloat16):
    level = level_of(key, shape, pieces, -0.22, 0.18) if pieces else 1.0
    drawn = jax.random.normal(key, shape, jnp.float32) * spread * level
    return jnp.minimum(jnp.maximum(drawn, -limit), limit).astype(dtype)


def setup_inputs(seed: int = 0, part: int = 0) -> dict:
    key_of = jax.random.split(jax.random.key(seed), 4)
    part_keys = jax.random.split(jax.random.fold_in(key_of[3], part), 4)
    basis_series = bell_draw(part_keys[0], (DETS, BASIS, NT), 1.0, 6.0, ((2, 16),))
    reconstruction = bell_draw(part_keys[1], (DETS, TEMPL, 2, BASIS), BASIS ** -0.5, 0.5, ((1, 8),))
    offsets = jax.random.randint(part_keys[2], (DETS,), T_DEV, MAXQ * T_DEV).astype(jnp.int32)
    return dict(basis_series=basis_series, reconstruction=reconstruction, offsets=offsets)


def reference(basis_series, reconstruction, offsets):
    slid_series = jnp.stack([jnp.roll(basis_series[detector], -offsets[detector], axis=1) for detector in range(DETS)])
    block_count = NT // T_DEV
    blocks = slid_series.reshape(DETS, BASIS, block_count, T_DEV).transpose(2, 0, 1, 3)

    def one_block(block):
        power_sum = jnp.zeros((TEMPL, T_DEV), jnp.float32)
        for detector in range(DETS):
            filtered = jnp.dot(reconstruction[detector].reshape(2 * TEMPL, BASIS), block[detector], preferred_element_type=jnp.float32)
            filtered = filtered.reshape(TEMPL, 2, T_DEV)
            power_sum = power_sum + lax.optimization_barrier(jnp.sum(filtered * filtered, axis=1))
        network = jnp.sqrt(power_sum)
        return lax.optimization_barrier(jnp.max(network.reshape(TEMPL, T_DEV // WIN, WIN), axis=2))
    peaks = lax.map(one_block, blocks)
    return peaks.transpose(1, 0, 2).reshape(TEMPL, NWIN)
```

```python
import functools
import math

import jax
import jax.numpy as jnp
from jax import lax
from jax.experimental import pallas as pl
from jax.experimental.pallas import tpu as pltpu
from jax.sharding import PartitionSpec as P

WIN = 128
MESH = pl.DeviceIdType.MESH
TINY = 1e-18
CODE = jnp.int16
SPAN = 30
STEPS = 1092
TOP = 15


def coded(power):
    log = jnp.log(jnp.maximum(power, 2.0 ** (TOP - 2 * SPAN))) * (STEPS / math.log(2.0))
    return jnp.round(log - (TOP - SPAN) * STEPS).astype(jnp.int32).astype(CODE)


def decoded(code):
    code = code.astype(jnp.int32).astype(jnp.float32)
    power = jnp.exp2(code * (1.0 / STEPS) + (TOP - SPAN))
    return jnp.where(code <= -SPAN * STEPS, 0.0, power)


def step_of(k, count):
    return count // 2 + (k // 2) * (2 * (k % 2) - 1)


def kernel(
    chips, cores,
    off_ref, basis_ref, bank_ref, out_ref,
    bank_all, stage, recv, dec, peaks, final,
    bank_s, bank_r, pow_s, pow_r, peak_s, peak_r,
):
    dets, basis, block = basis_ref.shape
    rows2 = bank_ref.shape[1] // cores
    rows = rows2 // 2
    half = block // 2
    wins = block // WIN
    count = chips * cores
    total = count * wins
    chip, core = lax.axis_index("tmpl"), lax.axis_index("det")
    me = chip * cores + core

    def dev(j, c):
        return {"tmpl": j, "det": c}

    top = jnp.max(jnp.abs(basis_ref[...]).astype(jnp.float32), axis=0)
    top = jnp.max(top, axis=0, keepdims=True)
    top = jnp.max(top, axis=1, keepdims=True)
    own = bank_ref[:, pl.ds(pl.multiple_of(core * rows2, rows2), rows2), :]
    bank_all[me, 0:dets] = own
    bank_all[me, dets] = jnp.broadcast_to(top, (rows2, WIN)).astype(jnp.bfloat16)
    own_max = jnp.max(jnp.max(jnp.max(jnp.abs(own).astype(jnp.float32), axis=0), axis=0, keepdims=True), axis=1, keepdims=True)

    barrier = pltpu.get_barrier_semaphore()

    @pl.loop(1, count)
    def _(k):
        t = lax.rem(me + k, count)
        pl.semaphore_signal(barrier, inc=1, device_id=dev(t // cores, lax.rem(t, cores)), device_id_type=MESH)

    pl.semaphore_wait(barrier, count - 1)

    def bank_copy(j, c, src):
        return pltpu.make_async_remote_copy(
            src_ref=bank_all.at[src], dst_ref=bank_all.at[src],
            send_sem=bank_s.at[j * cores + c], recv_sem=bank_r.at[src],
            device_id=dev(j, c), device_id_type=MESH)

    def pow_copy(j, c, src):
        return pltpu.make_async_remote_copy(
            src_ref=stage.at[j * cores + c], dst_ref=recv.at[src],
            send_sem=pow_s.at[j * cores + c], recv_sem=pow_r.at[src],
            device_id=dev(j, c), device_id_type=MESH)

    def peak_copy(j, c, src):
        return pltpu.make_async_remote_copy(
            src_ref=peaks.at[(j * cores + c) * wins // WIN], dst_ref=final.at[src],
            send_sem=peak_s.at[j * cores + c], recv_sem=peak_r.at[src],
            device_id=dev(j, c), device_id_type=MESH)

    def over_peers(fn, receive=False):
        for d in range(1, cores):
            fn(chip, lax.rem(core + d, cores))

        @pl.loop(1, chips)
        def _(k):
            s = step_of(k, chips)
            j = lax.rem(chip + chips - s, chips) if receive else lax.rem(chip + s, chips)
            for d in range(cores):
                fn(j, lax.rem(core + d, cores))

    over_peers(lambda j, c: bank_copy(j, c, me).start())

    size = cores * dets * rows2
    r = lax.broadcasted_iota(jnp.int32, (size, size), 0)
    i = lax.broadcasted_iota(jnp.int32, (size, size), 1)
    d_of = lax.div(r, cores * rows2)
    c_of = lax.rem(lax.div(r, rows2), cores)
    k_of = lax.rem(lax.div(r, rows), 2)
    m_of = lax.rem(r, rows)
    perm = (i == c_of * (dets * rows2) + d_of * rows2 + m_of * 2 + k_of).astype(jnp.float32).astype(jnp.bfloat16)

    def power_for(j):
        halves = [bank_all[j * cores + c, 0:dets].reshape(dets * rows2, basis) for c in range(cores)]
        invs = []
        for h in halves:
            b = jnp.max(jnp.abs(h).astype(jnp.float32), axis=0, keepdims=True)
            b = jnp.max(b, axis=1, keepdims=True)
            a = jnp.maximum(b * top, TINY)
            invs.append(1.0 / (a * a))
        w = jnp.dot(perm, jnp.concatenate(halves, axis=0), preferred_element_type=jnp.float32).astype(jnp.bfloat16)
        for d in range(dets):
            f = jnp.dot(w[d * cores * rows2:(d + 1) * cores * rows2], basis_ref[d], preferred_element_type=jnp.float32)
            f = f * f
            for c in range(cores):
                p = (f[c * rows2:c * rows2 + rows] + f[c * rows2 + rows:(c + 1) * rows2]) * invs[c]
                stage[j * cores + c, d] = coded(jnp.concatenate([p[:, :half], p[:, half:]], axis=0))

    for d in range(1, cores):
        bank_copy(chip, core, chip * cores + lax.rem(core + d, cores)).wait_recv()
    power_for(chip)
    for d in range(1, cores):
        pow_copy(chip, lax.rem(core + d, cores), me).start()

    @pl.loop(1, chips)
    def _(k):
        s = step_of(k, chips)
        j = lax.rem(chip + s, chips)
        for c in range(cores):
            bank_copy(chip, core, j * cores + c).wait_recv()
        power_for(j)
        for d in range(cores):
            pow_copy(j, lax.rem(core + d, cores), me).start()

    def decode(src, value):
        a = bank_all[src, dets].astype(jnp.float32)[0:rows]
        a = jnp.maximum(a * own_max, TINY)
        scale = a * a
        for d in range(dets):
            x = decoded(value(d))
            rest = lax.rem(off_ref[d], WIN)
            for v in range(wins):
                h, q = divmod(v, wins // 2)
                tile = x[h * rows:(h + 1) * rows, q * WIN:(q + 1) * WIN] * scale
                dec[d, src * wins + v] = pltpu.roll(tile, WIN - rest, 1)

    decode(me, lambda d: stage[me, d])

    def take(j, c):
        src = j * cores + c
        pow_copy(chip, core, src).wait_recv()
        decode(src, lambda d: recv[src, d])

    over_peers(take, receive=True)

    lane = lax.broadcasted_iota(jnp.int32, (rows, WIN), 1)
    shifts = [lax.div(off_ref[d], WIN) for d in range(dets)]
    keep = [lane < WIN - lax.rem(off_ref[d], WIN) for d in range(dets)]
    unroll = 16

    @pl.loop(0, total // WIN)
    def _(g):
        def body(u, acc):
            for v in range(unroll):
                at = u * unroll + v
                w = g * WIN + at
                power = None
                for d in range(dets):
                    first = lax.rem(w + shifts[d], total)
                    second = lax.rem(w + shifts[d] + 1, total)
                    x = jnp.where(keep[d], dec[d, first], dec[d, second])
                    power = x if power is None else power + x
                acc = jnp.where(lane == at, jnp.max(power, axis=1, keepdims=True), acc)
            return acc

        acc = lax.fori_loop(0, WIN // unroll, body, jnp.zeros((rows, WIN), jnp.float32))
        peaks[g] = jnp.sqrt(acc)

    over_peers(lambda j, c: peak_copy(j, c, me).start())

    def put(src, tile):
        tile = pltpu.roll(tile, lax.rem(WIN - lax.rem(me * wins, WIN), WIN), 1)
        out_ref[pl.ds(pl.multiple_of(src * rows, rows), rows), :] = tile[:, :wins]

    put(me, peaks[me * wins // WIN])

    def collect(j, c):
        src = j * cores + c
        peak_copy(chip, core, src).wait_recv()
        put(src, final[src])

    over_peers(collect, receive=True)

    def drain(j, c):
        bank_copy(j, c, me).wait_send()
        pow_copy(j, c, me).wait_send()
        peak_copy(j, c, me).wait_send()

    over_peers(drain)


def per_device(chips, cores, basis_series, reconstruction, offsets):
    dets, basis, block = basis_series.shape
    templates = reconstruction.shape[1]
    bank = reconstruction.reshape(dets, templates * 2, basis)
    count = chips * cores
    rows = templates // cores
    wins = block // WIN
    total = count * wins
    vmem = pl.BlockSpec(memory_space=pltpu.VMEM)
    return pl.pallas_call(
        functools.partial(kernel, chips, cores),
        out_shape=jax.ShapeDtypeStruct((count * rows, wins), jnp.float32),
        in_specs=[pl.BlockSpec(memory_space=pltpu.SMEM), vmem, vmem],
        out_specs=vmem,
        scratch_shapes=[
            pltpu.VMEM((count, dets + 1, rows * 2, basis), jnp.bfloat16),
            pltpu.VMEM((count, dets, rows * 2, block // 2), CODE),
            pltpu.VMEM((count, dets, rows * 2, block // 2), CODE),
            pltpu.VMEM((dets, total, rows, WIN), jnp.float32),
            pltpu.VMEM((max(total // WIN, 1), rows, WIN), jnp.float32),
            pltpu.VMEM((count, rows, WIN), jnp.float32),
        ] + [pltpu.SemaphoreType.DMA((count,)) for _ in range(6)],
        compiler_params=pltpu.CompilerParams(
            collective_id=0, has_side_effects=True, vmem_limit_bytes=63_000_000),
    )(offsets, basis_series, bank)


def solution(mesh):
    chips, cores = mesh.shape["tmpl"], mesh.shape["det"]
    in_specs = (
        P(None, None, ("groups", "tmpl", "det")),
        P(None, ("groups", "tmpl"), None, None),
        P("groups"),
    )
    out_specs = P(None, ("groups", "tmpl", "det"))
    return jax.shard_map(
        functools.partial(per_device, chips, cores),
        mesh=mesh, in_specs=in_specs, out_specs=out_specs, check_vma=False,
    )
```

```python
import functools
import math

import jax
import jax.numpy as jnp
from jax import lax
from jax.experimental import pallas as pl
from jax.experimental.pallas import tpu as pltpu
from jax.sharding import PartitionSpec as P

WIN = 128
SLIDE_BLOCKS = 16
MESH = pl.DeviceIdType.MESH
TINY = 1e-18
CODE = jnp.int16
SPAN = 30
STEPS = 1092
TOP = 15


def coded(power):
    log = jnp.log(jnp.maximum(power, 2.0 ** (TOP - 2 * SPAN))) * (STEPS / math.log(2.0))
    return jnp.round(log - (TOP - SPAN) * STEPS).astype(jnp.int32).astype(CODE)


def decoded(code):
    code = code.astype(jnp.int32).astype(jnp.float32)
    power = jnp.exp2(code * (1.0 / STEPS) + (TOP - SPAN))
    return jnp.where(code <= -SPAN * STEPS, 0.0, power)


def step_of(k, count):
    return count // 2 + (k // 2) * (2 * (k % 2) - 1)


def kernel(
    chips, cores,
    off_ref, basis_hbm, bank_hbm, out_ref,
    basis_ref, bank_ref, bank_all, top_all, stage, recv, dec, peaks, final,
    load, bank_s, bank_r, pass_s, top_s, top_r, pow_s, pow_r, peak_s, peak_r,
):
    dets, basis, block = basis_ref.shape
    rows2 = bank_ref.shape[1] // cores
    rows = rows2 // 2
    half = block // 2
    wins = block // WIN
    count = chips * cores
    total = count * wins
    per_row = WIN // rows
    chip, core = lax.axis_index("tmpl"), lax.axis_index("det")
    me = chip * cores + core

    load_bank = pltpu.make_async_copy(bank_hbm, bank_ref, load.at[0])
    load_basis = pltpu.make_async_copy(basis_hbm, basis_ref, load.at[1])
    load_bank.start()
    load_basis.start()

    def dev(j, c):
        return {"tmpl": j, "det": c}

    def over_chips(fn, receive=False):
        @pl.loop(1, chips)
        def _(k):
            s = step_of(k, chips)
            fn(lax.rem(chip + chips - s, chips) if receive else lax.rem(chip + s, chips))

    def over_peers(fn, receive=False):
        for d in range(1, cores):
            fn(chip, lax.rem(core + d, cores))

        def each(j):
            for d in range(cores):
                fn(j, lax.rem(core + d, cores))

        over_chips(each, receive)

    barrier = pltpu.get_barrier_semaphore()
    over_peers(lambda j, c: pl.semaphore_signal(barrier, inc=1, device_id=dev(j, c), device_id_type=MESH))

    mine = pl.ds(pl.multiple_of(core * rows2, rows2), rows2)

    def bank_copy(j, src):
        return pltpu.make_async_remote_copy(
            src_ref=bank_ref.at[:, mine], dst_ref=bank_all.at[src],
            send_sem=bank_s.at[j], recv_sem=bank_r.at[src],
            device_id=dev(j, core), device_id_type=MESH)

    def pass_copy(src, c):
        return pltpu.make_async_remote_copy(
            src_ref=bank_all.at[src], dst_ref=bank_all.at[src],
            send_sem=pass_s.at[lax.div(src, cores) * cores + c], recv_sem=bank_r.at[src],
            device_id=dev(chip, c), device_id_type=MESH)

    def top_copy(j, c, src):
        return pltpu.make_async_remote_copy(
            src_ref=top_all.at[src], dst_ref=top_all.at[src],
            send_sem=top_s.at[j * cores + c], recv_sem=top_r.at[src],
            device_id=dev(j, c), device_id_type=MESH)

    def pow_copy(j, c, src):
        return pltpu.make_async_remote_copy(
            src_ref=stage.at[j * cores + c], dst_ref=recv.at[src],
            send_sem=pow_s.at[j * cores + c], recv_sem=pow_r.at[src],
            device_id=dev(j, c), device_id_type=MESH)

    def peak_copy(j, c, src):
        return pltpu.make_async_remote_copy(
            src_ref=peaks.at[(j * cores + c) * wins // per_row], dst_ref=final.at[src],
            send_sem=peak_s.at[j * cores + c], recv_sem=peak_r.at[src],
            device_id=dev(j, c), device_id_type=MESH)

    size = cores * dets * rows2
    r = lax.broadcasted_iota(jnp.int32, (size, size), 0)
    i = lax.broadcasted_iota(jnp.int32, (size, size), 1)
    d_of = lax.div(r, cores * rows2)
    c_of = lax.rem(lax.div(r, rows2), cores)
    k_of = lax.rem(lax.div(r, rows), 2)
    m_of = lax.rem(r, rows)
    perm = (i == c_of * (dets * rows2) + d_of * rows2 + m_of * 2 + k_of).astype(jnp.float32).astype(jnp.bfloat16)

    def largest(x):
        x = jnp.max(jnp.abs(x).astype(jnp.float32), axis=0)
        return jnp.max(jnp.max(x, axis=0, keepdims=True), axis=1, keepdims=True)

    load_bank.wait()
    load_basis.wait()
    top = largest(basis_ref[...])
    top_all[me] = jnp.broadcast_to(top, (1, WIN))
    own_max = largest(bank_ref[:, mine])

    def power_for(j, halves):
        invs = []
        for h in halves:
            a = jnp.maximum(largest(h) * top, TINY)
            invs.append(1.0 / (a * a))
        w = jnp.concatenate([h.reshape(dets * rows2, basis) for h in halves], axis=0)
        w = jnp.dot(perm, w, preferred_element_type=jnp.float32).astype(jnp.bfloat16)
        for d in range(dets):
            f = jnp.dot(w[d * cores * rows2:(d + 1) * cores * rows2], basis_ref[d], preferred_element_type=jnp.float32)
            f = f * f
            for c in range(cores):
                p = (f[c * rows2:c * rows2 + rows] + f[c * rows2 + rows:(c + 1) * rows2]) * invs[c]
                stage[j * cores + c, d] = coded(jnp.concatenate([p[:, :half], p[:, half:]], axis=0))

    power_for(chip, [bank_ref[:, c * rows2:(c + 1) * rows2] for c in range(cores)])

    pl.semaphore_wait(barrier, count - 1)
    over_chips(lambda j: bank_copy(j, me).start())
    over_peers(lambda j, c: top_copy(j, c, me).start())
    for d in range(1, cores):
        pow_copy(chip, lax.rem(core + d, cores), me).start()

    def pass_on(k):
        src = lax.rem(chip + step_of(k, chips), chips) * cores + core
        bank_copy(chip, src).wait_recv()
        for d in range(1, cores):
            pass_copy(src, lax.rem(core + d, cores)).start()

    pass_on(1)

    @pl.loop(1, chips)
    def _(k):
        @pl.when(k < chips - 1)
        def _():
            pass_on(k + 1)

        j = lax.rem(chip + step_of(k, chips), chips)
        for d in range(1, cores):
            bank_copy(chip, j * cores + lax.rem(core + d, cores)).wait_recv()
        power_for(j, [bank_all[j * cores + c] for c in range(cores)])
        for d in range(cores):
            pow_copy(j, lax.rem(core + d, cores), me).start()

    rest = [lax.rem(off_ref[d], WIN) for d in range(dets)]
    shifts = [lax.div(off_ref[d], WIN) for d in range(dets)]

    def decode(src, value):
        a = jnp.maximum(top_all[src] * own_max, TINY)
        scale = a * a
        for d in range(dets):
            x = decoded(value(d))
            tiles = []
            for v in range(wins):
                h, q = divmod(v, wins // 2)
                tile = x[h * rows:(h + 1) * rows, q * WIN:(q + 1) * WIN] * scale
                tile = pltpu.roll(tile, WIN - rest[d], 1)
                dec[d, src * wins + v] = tile
                tiles.append(tile)

            @pl.when(src < SLIDE_BLOCKS)
            def _():
                for v in range(wins):
                    dec[d, (count + src) * wins + v] = tiles[v]

    decode(me, lambda d: stage[me, d])

    def take(j, c):
        src = j * cores + c
        top_copy(chip, core, src).wait_recv()
        pow_copy(chip, core, src).wait_recv()
        decode(src, lambda d: recv[src, d])

    over_peers(take, receive=True)

    lane = lax.broadcasted_iota(jnp.int32, (per_row, rows, WIN), 2)

    @pl.loop(0, total // per_row)
    def _(g):
        power = None
        for d in range(dets):
            tiles = dec[d, pl.ds(g * per_row + shifts[d], per_row + 1)]
            x = jnp.where(lane < WIN - rest[d], tiles[:per_row], tiles[1:])
            power = x if power is None else power + x
        turned = power.reshape(per_row * rows, WIN).T
        peaks[g] = jnp.sqrt(jnp.max(turned, axis=0, keepdims=True))

    over_peers(lambda j, c: peak_copy(j, c, me).start())
    final[me] = peaks[me * wins // per_row]
    over_peers(lambda j, c: peak_copy(chip, core, j * cores + c).wait_recv(), receive=True)

    base = lax.rem(me * wins, per_row) * rows
    e_of = lax.broadcasted_iota(jnp.int32, (per_row, WIN), 0)
    l_of = lax.broadcasted_iota(jnp.int32, (per_row, WIN), 1)
    for g in range(count // per_row):
        x = final[g * per_row:(g + 1) * per_row].reshape(per_row, WIN)
        x = pltpu.roll(x, lax.rem(WIN - base, WIN), 1)
        x = jnp.concatenate([
            pltpu.roll(x[h:h + 8], h * rows, 1, stride=rows, stride_axis=0) for h in range(0, per_row, 8)], axis=0)
        for i in range(wins):
            y = pltpu.roll(x, (WIN - i * rows) % WIN, 1)
            y = jnp.where(lax.div(l_of, rows) == e_of, y, 0.0)
            out_ref[i:i + 1, g * WIN:(g + 1) * WIN] = jnp.sum(y, axis=0, keepdims=True)

    over_chips(lambda j: bank_copy(j, me).wait_send())

    def passed(j):
        for d in range(1, cores):
            pass_copy(j * cores + core, lax.rem(core + d, cores)).wait_send()

    over_chips(passed)

    def drain(j, c):
        top_copy(j, c, me).wait_send()
        pow_copy(j, c, me).wait_send()
        peak_copy(j, c, me).wait_send()

    over_peers(drain)


def per_device(chips, cores, basis_series, reconstruction, offsets):
    dets, basis, block = basis_series.shape
    templates = reconstruction.shape[1]
    bank = reconstruction.reshape(dets, templates * 2, basis)
    count = chips * cores
    rows = templates // cores
    wins = block // WIN
    total = count * wins
    per_row = WIN // rows
    hbm = pl.BlockSpec(memory_space=pl.ANY)
    out = pl.pallas_call(
        functools.partial(kernel, chips, cores),
        out_shape=jax.ShapeDtypeStruct((wins, count * rows), jnp.float32),
        in_specs=[pl.BlockSpec(memory_space=pltpu.SMEM), hbm, hbm],
        out_specs=pl.BlockSpec(memory_space=pltpu.VMEM),
        scratch_shapes=[
            pltpu.VMEM(basis_series.shape, basis_series.dtype),
            pltpu.VMEM(bank.shape, bank.dtype),
            pltpu.VMEM((count, dets, rows * 2, basis), jnp.bfloat16),
            pltpu.VMEM((count, 1, WIN), jnp.float32),
            pltpu.VMEM((count, dets, rows * 2, block // 2), CODE),
            pltpu.VMEM((count, dets, rows * 2, block // 2), CODE),
            pltpu.VMEM((dets, total + SLIDE_BLOCKS * wins, rows, WIN), jnp.float32),
            pltpu.VMEM((total // per_row, 1, WIN), jnp.float32),
            pltpu.VMEM((count, 1, WIN), jnp.float32),
            pltpu.SemaphoreType.DMA((2,)),
            pltpu.SemaphoreType.DMA((chips,)),
        ] + [pltpu.SemaphoreType.DMA((count,)) for _ in range(8)],
        compiler_params=pltpu.CompilerParams(
            collective_id=0, has_side_effects=True, vmem_limit_bytes=63_000_000),
    )(offsets, basis_series, bank)
    return out.T


def solution(mesh):
    chips, cores = mesh.shape["tmpl"], mesh.shape["det"]
    in_specs = (
        P(None, None, ("groups", "tmpl", "det")),
        P(None, ("groups", "tmpl"), None, None),
        P("groups"),
    )
    out_specs = P(None, ("groups", "tmpl", "det"))
    return jax.shard_map(
        functools.partial(per_device, chips, cores),
        mesh=mesh, in_specs=in_specs, out_specs=out_specs, check_vma=False,
    )
```

```python
import functools
import math

import jax
import jax.numpy as jnp
from jax import lax
from jax.experimental import pallas as pl
from jax.experimental.pallas import tpu as pltpu
from jax.sharding import PartitionSpec as P

WIN = 128
SLIDE_BLOCKS = 16
MESH = pl.DeviceIdType.MESH
TINY = 1e-18
CODE = jnp.int16
SPAN = 30
STEPS = 1092
TOP = 15


def coded(power):
    log = jnp.log(jnp.maximum(power, 2.0 ** (TOP - 2 * SPAN))) * (STEPS / math.log(2.0))
    return jnp.round(log - (TOP - SPAN) * STEPS).astype(jnp.int32).astype(CODE)


def decoded(code):
    code = code.astype(jnp.int32).astype(jnp.float32)
    power = jnp.exp2(code * (1.0 / STEPS) + (TOP - SPAN))
    return jnp.where(code <= -SPAN * STEPS, 0.0, power)


def partner(chip, chips, k, sign):
    half = chips // 2
    near = k // half
    turn = k - near * half + near
    side = lax.rem(lax.div(chip, half) + 1 - near, 2)
    return side * half + lax.rem(lax.rem(chip, half) + half + sign * turn, half)


def kernel(
    chips, cores,
    off_ref, basis_hbm, bank_hbm, out_ref,
    basis_ref, bank_ref, bank_all, top_all, stage, recv, dec, peaks, final,
    load, bank_s, bank_r, pass_s, top_s, top_r, pow_s, pow_r, peak_s, peak_r,
):
    dets, basis, block = basis_ref.shape
    rows2 = bank_ref.shape[1] // cores
    rows = rows2 // 2
    half = block // 2
    wins = block // WIN
    count = chips * cores
    total = count * wins
    per_row = WIN // rows
    chip, core = lax.axis_index("tmpl"), lax.axis_index("det")
    me = chip * cores + core

    load_bank = pltpu.make_async_copy(bank_hbm, bank_ref, load.at[0])
    load_basis = pltpu.make_async_copy(basis_hbm, basis_ref, load.at[1])
    load_bank.start()
    load_basis.start()

    def dev(j, c):
        return {"tmpl": j, "det": c}

    def over_chips(fn, sign=1, short=True):
        if short and chips <= 8:
            for k in range(chips - 1):
                fn(partner(chip, chips, k, sign))
            return

        @pl.loop(0, chips - 1)
        def _(k):
            fn(partner(chip, chips, k, sign))

    def over_peers(fn, sign=1):
        for d in range(cores):
            over_chips(lambda j: fn(j, lax.rem(core + d, cores)), sign)
        for d in range(1, cores):
            fn(chip, lax.rem(core + d, cores))

    barrier = pltpu.get_barrier_semaphore()
    over_peers(lambda j, c: pl.semaphore_signal(barrier, inc=1, device_id=dev(j, c), device_id_type=MESH))

    mine = pl.ds(pl.multiple_of(core * rows2, rows2), rows2)

    def bank_copy(j, src):
        return pltpu.make_async_remote_copy(
            src_ref=bank_ref.at[:, mine], dst_ref=bank_all.at[src],
            send_sem=bank_s.at[j], recv_sem=bank_r.at[src],
            device_id=dev(j, core), device_id_type=MESH)

    def pass_copy(src, c):
        return pltpu.make_async_remote_copy(
            src_ref=bank_all.at[src], dst_ref=bank_all.at[src],
            send_sem=pass_s.at[lax.div(src, cores) * cores + c], recv_sem=bank_r.at[src],
            device_id=dev(chip, c), device_id_type=MESH)

    def top_copy(j, c, src):
        return pltpu.make_async_remote_copy(
            src_ref=top_all.at[src], dst_ref=top_all.at[src],
            send_sem=top_s.at[j * cores + c], recv_sem=top_r.at[src],
            device_id=dev(j, c), device_id_type=MESH)

    def pow_copy(j, c, src):
        return pltpu.make_async_remote_copy(
            src_ref=stage.at[j * cores + c], dst_ref=recv.at[src],
            send_sem=pow_s.at[j * cores + c], recv_sem=pow_r.at[src],
            device_id=dev(j, c), device_id_type=MESH)

    def peak_copy(j, c, src):
        return pltpu.make_async_remote_copy(
            src_ref=peaks.at[(j * cores + c) * wins // per_row], dst_ref=final.at[src],
            send_sem=peak_s.at[j * cores + c], recv_sem=peak_r.at[src],
            device_id=dev(j, c), device_id_type=MESH)

    r = lax.broadcasted_iota(jnp.int32, (dets * rows2, dets * rows2), 0)
    i = lax.broadcasted_iota(jnp.int32, (dets * rows2, dets * rows2), 1)
    d_of = lax.div(r, rows2)
    k_of = lax.rem(lax.div(r, rows), 2)
    m_of = lax.rem(r, rows)
    perm = (i == d_of * rows2 + m_of * 2 + k_of).astype(jnp.float32).astype(jnp.bfloat16)

    def largest(x):
        x = jnp.max(jnp.abs(x).astype(jnp.float32), axis=0)
        return jnp.max(jnp.max(x, axis=0, keepdims=True), axis=1, keepdims=True)

    load_bank.wait()
    load_basis.wait()
    top = largest(basis_ref[...])
    top_all[me] = jnp.broadcast_to(top, (1, WIN))
    own_max = largest(bank_ref[:, mine])

    def power_for(to, bank):
        a = jnp.maximum(largest(bank) * top, TINY)
        inv = 1.0 / (a * a)
        w = jnp.dot(perm, bank.reshape(dets * rows2, basis), preferred_element_type=jnp.float32).astype(jnp.bfloat16)
        for d in range(dets):
            f = jnp.dot(w[d * rows2:(d + 1) * rows2], basis_ref[d], preferred_element_type=jnp.float32)
            f = f * f
            p = (f[:rows] + f[rows:]) * inv
            stage[to, d] = coded(jnp.concatenate([p[:, :half], p[:, half:]], axis=0))

    for c in range(cores):
        power_for(chip * cores + c, bank_ref[:, c * rows2:(c + 1) * rows2])

    pl.semaphore_wait(barrier, count - 1)
    over_chips(lambda j: bank_copy(j, me).start())
    over_peers(lambda j, c: top_copy(j, c, me).start())
    for d in range(1, cores):
        pow_copy(chip, lax.rem(core + d, cores), me).start()

    def direct(j):
        src = j * cores + core
        bank_copy(chip, src).wait_recv()
        for d in range(1, cores):
            pass_copy(src, lax.rem(core + d, cores)).start()
        power_for(src, bank_all[src])
        pow_copy(j, core, me).start()

    over_chips(direct, -1, short=False)

    for d in range(1, cores):
        other = lax.rem(core + d, cores)

        def passed_on(j):
            src = j * cores + other
            bank_copy(chip, src).wait_recv()
            power_for(src, bank_all[src])
            pow_copy(j, other, me).start()

        over_chips(passed_on, -1, short=False)

    rest = [lax.rem(off_ref[d], WIN) for d in range(dets)]
    shifts = [lax.div(off_ref[d], WIN) for d in range(dets)]

    def decode(src, value):
        a = jnp.maximum(top_all[src] * own_max, TINY)
        scale = a * a
        for d in range(dets):
            x = decoded(value(d))
            tiles = []
            for v in range(wins):
                h, q = divmod(v, wins // 2)
                tile = x[h * rows:(h + 1) * rows, q * WIN:(q + 1) * WIN] * scale
                tile = pltpu.roll(tile, WIN - rest[d], 1)
                dec[d, src * wins + v] = tile
                tiles.append(tile)

            @pl.when(src < SLIDE_BLOCKS)
            def _():
                for v in range(wins):
                    dec[d, (count + src) * wins + v] = tiles[v]

    decode(me, lambda d: stage[me, d])

    def take(j, c):
        src = j * cores + c
        top_copy(chip, core, src).wait_recv()
        pow_copy(chip, core, src).wait_recv()
        decode(src, lambda d: recv[src, d])

    for d in range(1, cores):
        take(chip, lax.rem(core + d, cores))
    for d in range(cores):
        over_chips(lambda j: take(j, lax.rem(core + d, cores)), short=False)

    lane = lax.broadcasted_iota(jnp.int32, (per_row, rows, WIN), 2)

    @pl.loop(0, total // per_row, unroll=4)
    def _(g):
        power = None
        for d in range(dets):
            tiles = dec[d, pl.ds(g * per_row + shifts[d], per_row + 1)]
            x = jnp.where(lane < WIN - rest[d], tiles[:per_row], tiles[1:])
            power = x if power is None else power + x
        turned = power.reshape(per_row * rows, WIN).T
        peaks[g] = jnp.sqrt(jnp.max(turned, axis=0, keepdims=True))

    over_peers(lambda j, c: peak_copy(j, c, me).start())
    final[me] = peaks[me * wins // per_row]
    over_peers(lambda j, c: peak_copy(chip, core, j * cores + c).wait_recv(), -1)

    base = lax.rem(me * wins, per_row) * rows
    e_of = lax.broadcasted_iota(jnp.int32, (per_row, WIN), 0)
    l_of = lax.broadcasted_iota(jnp.int32, (per_row, WIN), 1)
    for g in range(count // per_row):
        x = final[g * per_row:(g + 1) * per_row].reshape(per_row, WIN)
        x = pltpu.roll(x, lax.rem(WIN - base, WIN), 1)
        x = jnp.concatenate([
            pltpu.roll(x[h:h + 8], h * rows, 1, stride=rows, stride_axis=0) for h in range(0, per_row, 8)], axis=0)
        for i in range(wins):
            y = pltpu.roll(x, (WIN - i * rows) % WIN, 1)
            y = jnp.where(lax.div(l_of, rows) == e_of, y, 0.0)
            out_ref[i:i + 1, g * WIN:(g + 1) * WIN] = jnp.sum(y, axis=0, keepdims=True)

    over_chips(lambda j: bank_copy(j, me).wait_send())

    def passed(j):
        for d in range(1, cores):
            pass_copy(j * cores + core, lax.rem(core + d, cores)).wait_send()

    over_chips(passed)

    def drain(j, c):
        top_copy(j, c, me).wait_send()
        pow_copy(j, c, me).wait_send()
        peak_copy(j, c, me).wait_send()

    over_peers(drain)


def per_device(chips, cores, basis_series, reconstruction, offsets):
    dets, basis, block = basis_series.shape
    templates = reconstruction.shape[1]
    bank = reconstruction.reshape(dets, templates * 2, basis)
    count = chips * cores
    rows = templates // cores
    wins = block // WIN
    total = count * wins
    per_row = WIN // rows
    hbm = pl.BlockSpec(memory_space=pl.ANY)
    out = pl.pallas_call(
        functools.partial(kernel, chips, cores),
        out_shape=jax.ShapeDtypeStruct((wins, count * rows), jnp.float32),
        in_specs=[pl.BlockSpec(memory_space=pltpu.SMEM), hbm, hbm],
        out_specs=pl.BlockSpec(memory_space=pltpu.VMEM),
        scratch_shapes=[
            pltpu.VMEM(basis_series.shape, basis_series.dtype),
            pltpu.VMEM(bank.shape, bank.dtype),
            pltpu.VMEM((count, dets, rows * 2, basis), jnp.bfloat16),
            pltpu.VMEM((count, 1, WIN), jnp.float32),
            pltpu.VMEM((count, dets, rows * 2, block // 2), CODE),
            pltpu.VMEM((count, dets, rows * 2, block // 2), CODE),
            pltpu.VMEM((dets, total + SLIDE_BLOCKS * wins, rows, WIN), jnp.float32),
            pltpu.VMEM((total // per_row, 1, WIN), jnp.float32),
            pltpu.VMEM((count, 1, WIN), jnp.float32),
            pltpu.SemaphoreType.DMA((2,)),
            pltpu.SemaphoreType.DMA((chips,)),
        ] + [pltpu.SemaphoreType.DMA((count,)) for _ in range(8)],
        compiler_params=pltpu.CompilerParams(
            collective_id=0, has_side_effects=True, vmem_limit_bytes=63_000_000),
    )(offsets, basis_series, bank)
    return out.T


def solution(mesh):
    chips, cores = mesh.shape["tmpl"], mesh.shape["det"]
    in_specs = (
        P(None, None, ("groups", "tmpl", "det")),
        P(None, ("groups", "tmpl"), None, None),
        P("groups"),
    )
    out_specs = P(None, ("groups", "tmpl", "det"))
    return jax.shard_map(
        functools.partial(per_device, chips, cores),
        mesh=mesh, in_specs=in_specs, out_specs=out_specs, check_vma=False,
    )
```

```python
import functools
import math

import jax
import jax.numpy as jnp
from jax import lax
from jax.experimental import pallas as pl
from jax.experimental.pallas import tpu as pltpu
from jax.sharding import PartitionSpec as P

WIN = 128
SLIDE_BLOCKS = 16
MESH = pl.DeviceIdType.MESH
TINY = 1e-18
CODE = jnp.int16
SPAN = 30
STEPS = 1092
TOP = 15


def coded(power):
    log = jnp.log(jnp.maximum(power, 2.0 ** (TOP - 2 * SPAN))) * (STEPS / math.log(2.0))
    return jnp.round(log - (TOP - SPAN) * STEPS).astype(jnp.int32).astype(CODE)


def decoded(code):
    code = code.astype(jnp.int32).astype(jnp.float32)
    power = jnp.exp2(code * (1.0 / STEPS) + (TOP - SPAN))
    return jnp.where(code <= -SPAN * STEPS, 0.0, power)


def partner(chip, chips, k, sign):
    half = chips // 2
    near = k // half
    turn = k - near * half + near
    side = lax.rem(lax.div(chip, half) + 1 - near, 2)
    return side * half + lax.rem(lax.rem(chip, half) + half + sign * turn, half)


def kernel(
    chips, cores,
    off_hbm, basis_hbm, bank_hbm, out_ref,
    off_ref, basis_ref, bank_ref, bank_all, top_all, stage, recv, dec, peaks, final,
    load, bank_s, bank_r, pass_s, top_s, top_r, pow_s, pow_r, peak_s, peak_r,
):
    dets, basis, block = basis_ref.shape
    rows2 = bank_ref.shape[1] // cores
    rows = rows2 // 2
    half = block // 2
    wins = block // WIN
    count = chips * cores
    total = count * wins
    per_row = WIN // rows
    chip, core = lax.axis_index("tmpl"), lax.axis_index("det")
    me = chip * cores + core

    load_bank = pltpu.make_async_copy(bank_hbm, bank_ref, load.at[0])
    load_basis = pltpu.make_async_copy(basis_hbm, basis_ref, load.at[1])
    load_off = pltpu.make_async_copy(off_hbm, off_ref, load.at[2])
    load_bank.start()
    load_basis.start()
    load_off.start()

    def dev(j, c):
        return {"tmpl": j, "det": c}

    def over_chips(fn, sign=1, short=True):
        if short and chips <= 8:
            for k in range(chips - 1):
                fn(partner(chip, chips, k, sign))
            return

        @pl.loop(0, chips - 1)
        def _(k):
            fn(partner(chip, chips, k, sign))

    def over_peers(fn, sign=1):
        for d in range(cores):
            over_chips(lambda j: fn(j, lax.rem(core + d, cores)), sign)
        for d in range(1, cores):
            fn(chip, lax.rem(core + d, cores))

    barrier = pltpu.get_barrier_semaphore()
    over_peers(lambda j, c: pl.semaphore_signal(barrier, inc=1, device_id=dev(j, c), device_id_type=MESH))

    mine = pl.ds(pl.multiple_of(core * rows2, rows2), rows2)

    def bank_copy(j, src):
        return pltpu.make_async_remote_copy(
            src_ref=bank_ref.at[:, mine], dst_ref=bank_all.at[src],
            send_sem=bank_s.at[j], recv_sem=bank_r.at[src],
            device_id=dev(j, core), device_id_type=MESH)

    def pass_copy(src, c):
        return pltpu.make_async_remote_copy(
            src_ref=bank_all.at[src], dst_ref=bank_all.at[src],
            send_sem=pass_s.at[lax.div(src, cores) * cores + c], recv_sem=bank_r.at[src],
            device_id=dev(chip, c), device_id_type=MESH)

    def top_copy(j, c, src):
        return pltpu.make_async_remote_copy(
            src_ref=top_all.at[src], dst_ref=top_all.at[src],
            send_sem=top_s.at[j * cores + c], recv_sem=top_r.at[src],
            device_id=dev(j, c), device_id_type=MESH)

    def pow_copy(j, c, src):
        return pltpu.make_async_remote_copy(
            src_ref=stage.at[j * cores + c], dst_ref=recv.at[src],
            send_sem=pow_s.at[j * cores + c], recv_sem=pow_r.at[src],
            device_id=dev(j, c), device_id_type=MESH)

    def peak_copy(j, c, src):
        return pltpu.make_async_remote_copy(
            src_ref=peaks.at[(j * cores + c) * wins // per_row], dst_ref=final.at[src],
            send_sem=peak_s.at[j * cores + c], recv_sem=peak_r.at[src],
            device_id=dev(j, c), device_id_type=MESH)

    r = lax.broadcasted_iota(jnp.int32, (dets * rows2, dets * rows2), 0)
    i = lax.broadcasted_iota(jnp.int32, (dets * rows2, dets * rows2), 1)
    d_of = lax.div(r, rows2)
    k_of = lax.rem(lax.div(r, rows), 2)
    m_of = lax.rem(r, rows)
    perm = (i == d_of * rows2 + m_of * 2 + k_of).astype(jnp.float32).astype(jnp.bfloat16)

    def largest(x):
        x = jnp.max(jnp.abs(x).astype(jnp.float32), axis=0)
        return jnp.max(jnp.max(x, axis=0, keepdims=True), axis=1, keepdims=True)

    load_bank.wait()
    load_basis.wait()
    load_off.wait()
    top = largest(basis_ref[...])
    top_all[me] = jnp.broadcast_to(top, (1, WIN))
    own_max = largest(bank_ref[:, mine])

    def power_for(to, bank):
        a = jnp.maximum(largest(bank) * top, TINY)
        inv = 1.0 / (a * a)
        w = jnp.dot(perm, bank.reshape(dets * rows2, basis), preferred_element_type=jnp.float32).astype(jnp.bfloat16)
        for d in range(dets):
            f = jnp.dot(w[d * rows2:(d + 1) * rows2], basis_ref[d], preferred_element_type=jnp.float32)
            f = f * f
            p = (f[:rows] + f[rows:]) * inv
            stage[to, d] = coded(jnp.concatenate([p[:, :half], p[:, half:]], axis=0))

    for c in range(cores):
        power_for(chip * cores + c, bank_ref[:, c * rows2:(c + 1) * rows2])

    pl.semaphore_wait(barrier, count - 1)
    over_chips(lambda j: bank_copy(j, me).start())
    over_peers(lambda j, c: top_copy(j, c, me).start())
    for d in range(1, cores):
        pow_copy(chip, lax.rem(core + d, cores), me).start()

    def direct(j):
        src = j * cores + core
        bank_copy(chip, src).wait_recv()
        for d in range(1, cores):
            pass_copy(src, lax.rem(core + d, cores)).start()
        power_for(src, bank_all[src])
        pow_copy(j, core, me).start()

    over_chips(direct, -1, short=False)

    for d in range(1, cores):
        other = lax.rem(core + d, cores)

        def passed_on(j):
            src = j * cores + other
            bank_copy(chip, src).wait_recv()
            power_for(src, bank_all[src])
            pow_copy(j, other, me).start()

        over_chips(passed_on, -1, short=False)

    rest = [lax.rem(off_ref[d], WIN) for d in range(dets)]
    shifts = [lax.div(off_ref[d], WIN) for d in range(dets)]

    def decode(src, value):
        a = jnp.maximum(top_all[src] * own_max, TINY)
        scale = a * a
        for d in range(dets):
            x = decoded(value(d))
            tiles = []
            for v in range(wins):
                h, q = divmod(v, wins // 2)
                tile = x[h * rows:(h + 1) * rows, q * WIN:(q + 1) * WIN] * scale
                tile = pltpu.roll(tile, WIN - rest[d], 1)
                dec[d, src * wins + v] = tile
                tiles.append(tile)

            @pl.when(src < SLIDE_BLOCKS)
            def _():
                for v in range(wins):
                    dec[d, (count + src) * wins + v] = tiles[v]

    decode(me, lambda d: stage[me, d])

    def take(j, c):
        src = j * cores + c
        top_copy(chip, core, src).wait_recv()
        pow_copy(chip, core, src).wait_recv()
        decode(src, lambda d: recv[src, d])

    for d in range(1, cores):
        take(chip, lax.rem(core + d, cores))
    for d in range(cores):
        over_chips(lambda j: take(j, lax.rem(core + d, cores)), short=False)

    lane = lax.broadcasted_iota(jnp.int32, (per_row, rows, WIN), 2)

    @pl.loop(0, total // per_row, unroll=4)
    def _(g):
        power = None
        for d in range(dets):
            tiles = dec[d, pl.ds(g * per_row + shifts[d], per_row + 1)]
            x = jnp.where(lane < WIN - rest[d], tiles[:per_row], tiles[1:])
            power = x if power is None else power + x
        turned = power.reshape(per_row * rows, WIN).T
        peaks[g] = jnp.sqrt(jnp.max(turned, axis=0, keepdims=True))

    over_peers(lambda j, c: peak_copy(j, c, me).start())
    final[me] = peaks[me * wins // per_row]
    over_peers(lambda j, c: peak_copy(chip, core, j * cores + c).wait_recv(), -1)

    base = lax.rem(me * wins, per_row) * rows
    e_of = lax.broadcasted_iota(jnp.int32, (per_row, WIN), 0)
    l_of = lax.broadcasted_iota(jnp.int32, (per_row, WIN), 1)
    for g in range(count // per_row):
        x = final[g * per_row:(g + 1) * per_row].reshape(per_row, WIN)
        x = pltpu.roll(x, lax.rem(WIN - base, WIN), 1)
        x = jnp.concatenate([
            pltpu.roll(x[h:h + 8], h * rows, 1, stride=rows, stride_axis=0) for h in range(0, per_row, 8)], axis=0)
        for i in range(wins):
            y = pltpu.roll(x, (WIN - i * rows) % WIN, 1)
            y = jnp.where(lax.div(l_of, rows) == e_of, y, 0.0)
            out_ref[i:i + 1, g * WIN:(g + 1) * WIN] = jnp.sum(y, axis=0, keepdims=True)

    over_chips(lambda j: bank_copy(j, me).wait_send())

    def passed(j):
        for d in range(1, cores):
            pass_copy(j * cores + core, lax.rem(core + d, cores)).wait_send()

    over_chips(passed)

    def drain(j, c):
        top_copy(j, c, me).wait_send()
        pow_copy(j, c, me).wait_send()
        peak_copy(j, c, me).wait_send()

    over_peers(drain)


def per_device(chips, cores, basis_series, reconstruction, offsets):
    dets, basis, block = basis_series.shape
    templates = reconstruction.shape[1]
    bank = reconstruction.reshape(dets, templates * 2, basis)
    count = chips * cores
    rows = templates // cores
    wins = block // WIN
    total = count * wins
    per_row = WIN // rows
    hbm = pl.BlockSpec(memory_space=pltpu.HBM)
    out = pl.pallas_call(
        functools.partial(kernel, chips, cores),
        out_shape=jax.ShapeDtypeStruct((wins, count * rows), jnp.float32),
        in_specs=[hbm, hbm, hbm],
        out_specs=pl.BlockSpec(memory_space=pltpu.VMEM),
        scratch_shapes=[
            pltpu.SMEM(offsets.shape, offsets.dtype),
            pltpu.VMEM(basis_series.shape, basis_series.dtype),
            pltpu.VMEM(bank.shape, bank.dtype),
            pltpu.VMEM((count, dets, rows * 2, basis), jnp.bfloat16),
            pltpu.VMEM((count, 1, WIN), jnp.float32),
            pltpu.VMEM((count, dets, rows * 2, block // 2), CODE),
            pltpu.VMEM((count, dets, rows * 2, block // 2), CODE),
            pltpu.VMEM((dets, total + SLIDE_BLOCKS * wins, rows, WIN), jnp.float32),
            pltpu.VMEM((total // per_row, 1, WIN), jnp.float32),
            pltpu.VMEM((count, 1, WIN), jnp.float32),
            pltpu.SemaphoreType.DMA((3,)),
            pltpu.SemaphoreType.DMA((chips,)),
        ] + [pltpu.SemaphoreType.DMA((count,)) for _ in range(8)],
        compiler_params=pltpu.CompilerParams(
            collective_id=0, has_side_effects=True, vmem_limit_bytes=63_000_000),
    )(offsets, basis_series, bank)
    return out.T


def solution(mesh):
    chips, cores = mesh.shape["tmpl"], mesh.shape["det"]
    in_specs = (
        P(None, None, ("groups", "tmpl", "det")),
        P(None, ("groups", "tmpl"), None, None),
        P("groups"),
    )
    out_specs = P(None, ("groups", "tmpl", "det"))
    return jax.shard_map(
        functools.partial(per_device, chips, cores),
        mesh=mesh, in_specs=in_specs, out_specs=out_specs, check_vma=False,
    )
```

```python
import functools
import math

import jax
import jax.numpy as jnp
from jax import lax
from jax.experimental import pallas as pl
from jax.experimental.pallas import tpu as pltpu
from jax.sharding import PartitionSpec as P

WIN = 128
SLIDE_BLOCKS = 16
MESH = pl.DeviceIdType.MESH
TINY = 1e-18
CODE = jnp.int16
SPAN = 30
STEPS = 1092
TOP = 15


def coded(power):
    log = jnp.log(jnp.maximum(power, 2.0 ** (TOP - 2 * SPAN))) * (STEPS / math.log(2.0))
    return jnp.round(log - (TOP - SPAN) * STEPS).astype(jnp.int32).astype(CODE)


def decoded(code):
    code = code.astype(jnp.int32).astype(jnp.float32)
    power = jnp.exp2(code * (1.0 / STEPS) + (TOP - SPAN))
    return jnp.where(code <= -SPAN * STEPS, 0.0, power)


def partner(chip, chips, k, sign):
    half = chips // 2
    near = k // half
    turn = k - near * half + near
    side = lax.rem(lax.div(chip, half) + 1 - near, 2)
    return side * half + lax.rem(lax.rem(chip, half) + half + sign * turn, half)


def kernel(
    chips, cores,
    off_hbm, basis_hbm, bank_hbm, out_ref,
    off_ref, basis_ref, bank_ref, bank_all, top_all, stage, recv, dec, peaks, final,
    load, bank_s, bank_r, pass_s, top_s, top_r, pow_s, pow_r, peak_s, peak_r,
):
    dets, basis, block = basis_ref.shape
    rows2 = bank_ref.shape[1] // cores
    rows = rows2 // 2
    half = block // 2
    wins = block // WIN
    count = chips * cores
    total = count * wins
    per_row = WIN // rows
    chip, core = lax.axis_index("tmpl"), lax.axis_index("det")
    me = chip * cores + core

    load_bank = pltpu.make_async_copy(bank_hbm, bank_ref, load.at[0])
    load_basis = pltpu.make_async_copy(basis_hbm, basis_ref, load.at[1])
    load_off = pltpu.make_async_copy(off_hbm, off_ref, load.at[2])
    load_bank.start()
    load_basis.start()
    load_off.start()

    def dev(j, c):
        return {"tmpl": j, "det": c}

    def over_chips(fn, sign=1, short=True):
        if short and chips <= 8:
            for k in range(chips - 1):
                fn(partner(chip, chips, k, sign))
            return

        @pl.loop(0, chips - 1)
        def _(k):
            fn(partner(chip, chips, k, sign))

    def over_peers(fn, sign=1):
        for d in range(cores):
            over_chips(lambda j: fn(j, lax.rem(core + d, cores)), sign)
        for d in range(1, cores):
            fn(chip, lax.rem(core + d, cores))

    barrier = pltpu.get_barrier_semaphore()
    over_peers(lambda j, c: pl.semaphore_signal(barrier, inc=1, device_id=dev(j, c), device_id_type=MESH))

    mine = pl.ds(pl.multiple_of(core * rows2, rows2), rows2)

    def bank_copy(j, src):
        return pltpu.make_async_remote_copy(
            src_ref=bank_ref.at[:, mine], dst_ref=bank_all.at[src],
            send_sem=bank_s.at[j], recv_sem=bank_r.at[src],
            device_id=dev(j, core), device_id_type=MESH)

    def pass_copy(src, c):
        return pltpu.make_async_remote_copy(
            src_ref=bank_all.at[src], dst_ref=bank_all.at[src],
            send_sem=pass_s.at[lax.div(src, cores) * cores + c], recv_sem=bank_r.at[src],
            device_id=dev(chip, c), device_id_type=MESH)

    def top_copy(j, c, src):
        return pltpu.make_async_remote_copy(
            src_ref=top_all.at[src], dst_ref=top_all.at[src],
            send_sem=top_s.at[j * cores + c], recv_sem=top_r.at[src],
            device_id=dev(j, c), device_id_type=MESH)

    def pow_copy(j, c, src):
        return pltpu.make_async_remote_copy(
            src_ref=stage.at[j * cores + c], dst_ref=recv.at[src],
            send_sem=pow_s.at[j * cores + c], recv_sem=pow_r.at[src],
            device_id=dev(j, c), device_id_type=MESH)

    def peak_copy(j, c, src):
        return pltpu.make_async_remote_copy(
            src_ref=peaks.at[(j * cores + c) * wins // per_row], dst_ref=final.at[src],
            send_sem=peak_s.at[j * cores + c], recv_sem=peak_r.at[src],
            device_id=dev(j, c), device_id_type=MESH)

    r = lax.broadcasted_iota(jnp.int32, (dets * rows2, dets * rows2), 0)
    i = lax.broadcasted_iota(jnp.int32, (dets * rows2, dets * rows2), 1)
    d_of = lax.div(r, rows2)
    k_of = lax.rem(lax.div(r, rows), 2)
    m_of = lax.rem(r, rows)
    perm = (i == d_of * rows2 + m_of * 2 + k_of).astype(jnp.float32).astype(jnp.bfloat16)

    def largest(x):
        x = jnp.max(jnp.abs(x).astype(jnp.float32), axis=0)
        return jnp.max(jnp.max(x, axis=0, keepdims=True), axis=1, keepdims=True)

    load_bank.wait()
    load_basis.wait()
    load_off.wait()
    top = largest(basis_ref[...])
    top_all[me] = jnp.broadcast_to(top, (1, WIN))
    own_max = largest(bank_ref[:, mine])

    def power_for(to, bank):
        a = jnp.maximum(largest(bank) * top, TINY)
        inv = 1.0 / (a * a)
        w = jnp.dot(perm, bank.reshape(dets * rows2, basis), preferred_element_type=jnp.float32).astype(jnp.bfloat16)
        for d in range(dets):
            f = jnp.dot(w[d * rows2:(d + 1) * rows2], basis_ref[d], preferred_element_type=jnp.float32)
            f = f * f
            p = (f[:rows] + f[rows:]) * inv
            stage[to, d] = coded(jnp.concatenate([p[:, :half], p[:, half:]], axis=0))

    for c in range(cores):
        power_for(chip * cores + c, bank_ref[:, c * rows2:(c + 1) * rows2])

    pl.semaphore_wait(barrier, count - 1)
    over_chips(lambda j: bank_copy(j, me).start())
    over_peers(lambda j, c: top_copy(j, c, me).start())
    for d in range(1, cores):
        pow_copy(chip, lax.rem(core + d, cores), me).start()

    def direct(j):
        src = j * cores + core
        bank_copy(chip, src).wait_recv()
        for d in range(1, cores):
            pass_copy(src, lax.rem(core + d, cores)).start()
        power_for(src, bank_all[src])
        pow_copy(j, core, me).start()

    over_chips(direct, -1, short=False)

    for d in range(1, cores):
        other = lax.rem(core + d, cores)

        def passed_on(j):
            src = j * cores + other
            bank_copy(chip, src).wait_recv()
            power_for(src, bank_all[src])
            pow_copy(j, other, me).start()

        over_chips(passed_on, -1, short=False)

    rest = [lax.rem(off_ref[d], WIN) for d in range(dets)]
    shifts = [lax.div(off_ref[d], WIN) for d in range(dets)]

    def decode(src, value):
        a = jnp.maximum(top_all[src] * own_max, TINY)
        scale = a * a
        for d in range(dets):
            x = decoded(value(d))
            tiles = []
            for v in range(wins):
                h, q = divmod(v, wins // 2)
                tile = x[h * rows:(h + 1) * rows, q * WIN:(q + 1) * WIN] * scale
                tile = pltpu.roll(tile, WIN - rest[d], 1)
                dec[d, src * wins + v] = tile
                tiles.append(tile)

            @pl.when(src < SLIDE_BLOCKS)
            def _():
                for v in range(wins):
                    dec[d, (count + src) * wins + v] = tiles[v]

    decode(me, lambda d: stage[me, d])

    def take(j, c):
        src = j * cores + c
        top_copy(chip, core, src).wait_recv()
        pow_copy(chip, core, src).wait_recv()
        decode(src, lambda d: recv[src, d])

    for d in range(1, cores):
        take(chip, lax.rem(core + d, cores))
    for d in range(cores):
        over_chips(lambda j: take(j, lax.rem(core + d, cores)), short=False)

    lane = lax.broadcasted_iota(jnp.int32, (per_row, rows, WIN), 2)

    @pl.loop(0, total // per_row, unroll=8)
    def _(g):
        power = None
        for d in range(dets):
            tiles = dec[d, pl.ds(g * per_row + shifts[d], per_row + 1)]
            x = jnp.where(lane < WIN - rest[d], tiles[:per_row], tiles[1:])
            power = x if power is None else power + x
        turned = power.reshape(per_row * rows, WIN).T
        peaks[g] = jnp.sqrt(jnp.max(turned, axis=0, keepdims=True))

    over_peers(lambda j, c: peak_copy(j, c, me).start())
    final[me] = peaks[me * wins // per_row]
    over_peers(lambda j, c: peak_copy(chip, core, j * cores + c).wait_recv(), -1)

    base = lax.rem(me * wins, per_row) * rows
    e_of = lax.broadcasted_iota(jnp.int32, (per_row, WIN), 0)
    l_of = lax.broadcasted_iota(jnp.int32, (per_row, WIN), 1)
    for g in range(count // per_row):
        x = final[g * per_row:(g + 1) * per_row].reshape(per_row, WIN)
        x = pltpu.roll(x, lax.rem(WIN - base, WIN), 1)
        x = jnp.concatenate([
            pltpu.roll(x[h:h + 8], h * rows, 1, stride=rows, stride_axis=0) for h in range(0, per_row, 8)], axis=0)
        for i in range(wins):
            y = pltpu.roll(x, (WIN - i * rows) % WIN, 1)
            y = jnp.where(lax.div(l_of, rows) == e_of, y, 0.0)
            out_ref[i:i + 1, g * WIN:(g + 1) * WIN] = jnp.sum(y, axis=0, keepdims=True)

    over_chips(lambda j: bank_copy(j, me).wait_send())

    def passed(j):
        for d in range(1, cores):
            pass_copy(j * cores + core, lax.rem(core + d, cores)).wait_send()

    over_chips(passed)

    def drain(j, c):
        top_copy(j, c, me).wait_send()
        pow_copy(j, c, me).wait_send()
        peak_copy(j, c, me).wait_send()

    over_peers(drain)


def per_device(chips, cores, basis_series, reconstruction, offsets):
    dets, basis, block = basis_series.shape
    templates = reconstruction.shape[1]
    bank = reconstruction.reshape(dets, templates * 2, basis)
    count = chips * cores
    rows = templates // cores
    wins = block // WIN
    total = count * wins
    per_row = WIN // rows
    hbm = pl.BlockSpec(memory_space=pltpu.HBM)
    out = pl.pallas_call(
        functools.partial(kernel, chips, cores),
        out_shape=jax.ShapeDtypeStruct((wins, count * rows), jnp.float32),
        in_specs=[hbm, hbm, hbm],
        out_specs=pl.BlockSpec(memory_space=pltpu.VMEM),
        scratch_shapes=[
            pltpu.SMEM(offsets.shape, offsets.dtype),
            pltpu.VMEM(basis_series.shape, basis_series.dtype),
            pltpu.VMEM(bank.shape, bank.dtype),
            pltpu.VMEM((count, dets, rows * 2, basis), jnp.bfloat16),
            pltpu.VMEM((count, 1, WIN), jnp.float32),
            pltpu.VMEM((count, dets, rows * 2, block // 2), CODE),
            pltpu.VMEM((count, dets, rows * 2, block // 2), CODE),
            pltpu.VMEM((dets, total + SLIDE_BLOCKS * wins, rows, WIN), jnp.float32),
            pltpu.VMEM((total // per_row, 1, WIN), jnp.float32),
            pltpu.VMEM((count, 1, WIN), jnp.float32),
            pltpu.SemaphoreType.DMA((3,)),
            pltpu.SemaphoreType.DMA((chips,)),
        ] + [pltpu.SemaphoreType.DMA((count,)) for _ in range(8)],
        compiler_params=pltpu.CompilerParams(
            collective_id=0, has_side_effects=True, vmem_limit_bytes=63_000_000),
    )(offsets, basis_series, bank)
    return out.T


def solution(mesh):
    chips, cores = mesh.shape["tmpl"], mesh.shape["det"]
    in_specs = (
        P(None, None, ("groups", "tmpl", "det")),
        P(None, ("groups", "tmpl"), None, None),
        P("groups"),
    )
    out_specs = P(None, ("groups", "tmpl", "det"))
    return jax.shard_map(
        functools.partial(per_device, chips, cores),
        mesh=mesh, in_specs=in_specs, out_specs=out_specs, check_vma=False,
    )
```
